32 devices in a mesh: tok: 8 (over z, y), vocab: 4 (over x, core).
Axes of the slice: x: 2, y: 2, z: 4, core: 2. Of those that a mesh axis runs over, the one named last changes fastest.
Arguments:
- hidden: bfloat16 [192, 9216], P('tok'), may hold values from -256 to 256
- policy_head: bfloat16 [9216, 32768], P(None, ('tok', 'vocab')), may hold values from -0.0625 to 0.0625
- reference_head: bfloat16 [9216, 32768], P(None, ('tok', 'vocab')), may hold values from -0.0625 to 0.0625
- targets: int32 [192], P('tok'), may hold values from 0 to 32767
Outputs:
- policy_logprob: float32 [192], P('tok')
- reference_logprob: float32 [192], P('tok')
- divergence: float32 [192], P('tok')
The draws below stay inside these ranges and needn't reach their ends.
All inputs are finite; a program needn't handle non-finite values.
Results may differ from the reference program's by a relative error of at most 0.00055.
Values may be sent and summed in bfloat16 or wider, within the bound.
A program may use at most 128 MiB of HBM per device.

```python
import math
import jax
import jax.numpy as jnp
import numpy as np

D = 9216
TOKENS = 192
V = 32768


def draw_hidden(key, part):
    key_base, key_scale = jax.random.split(key, 2)
    base = jax.random.normal(key_base, (TOKENS, D), jnp.float32)
    base = jnp.clip(base, -6.0, 6.0)
    scales = jnp.exp(jax.random.uniform(key_scale, (TOKENS, 1), jnp.float32, 0.0, math.log(4.0)))
    return (base * scales).astype(jnp.bfloat16)


def plant(entries, rng, smallest, top_value):
    longest = entries.shape.index(max(entries.shape))
    spots = []
    for shift in (0, 1):
        where = [jax.random.randint(jax.random.fold_in(rng, axis), (), 0, length) for axis, length in enumerate(entries.shape)]
        where[longest] = (where[longest] + shift) % entries.shape[longest]
        spots.append(tuple(where))
    return entries.at[spots[0]].set(smallest).at[spots[1]].set(top_value)


def block_levels(own_key, dims, cuts, smallest, top_value):
    gain = 1.0
    for position, blocks in cuts:
        steps = jax.random.uniform(jax.random.fold_in(jax.random.fold_in(own_key, 6), position), (blocks,), jnp.float32, smallest / len(cuts), top_value / len(cuts))
        gain = gain * jnp.repeat(jnp.exp(steps), dims[position] // blocks).reshape((-1,) + (1,) * (len(dims) - 1 - position))
    return gain


def rank_table(amount, slope):
    loads = [(1 << 20) // math.isqrt(standing ** slope) + 1 for standing in range(1, amount + 1)]
    scale = 1 + sum(loads) // (1 << 30)
    return np.cumsum(np.array([max(1, weight // scale) for weight in loads]))


def ranked_ids(key, dims, number_of, slope):
    table = rank_table(number_of, slope)
    ticket = jax.random.randint(jax.random.fold_in(key, 1), dims, 0, int(table[number_of - 1]))
    grade = jnp.searchsorted(jnp.asarray(table, jnp.int32), ticket, side="right")
    return jax.random.permutation(jax.random.fold_in(key, 2), number_of)[grade].astype(jnp.int32)


def scatter_about(stream_key, extent, spread, reach, pieces=(), kind=jnp.bfloat16):
    result = jax.random.normal(stream_key, extent, jnp.float32) * spread
    if len(pieces) > 0:
        result = block_levels(stream_key, extent, pieces, -0.22, 0.18) * result
    return jnp.clip(result, min=-reach, max=reach).astype(kind)


def setup_inputs(seed: int = 0) -> dict:
    splits = jax.random.split(jax.random.key(seed), 5)
    return {
        "hidden": draw_hidden(jax.random.fold_in(splits[4], 71), 0),
        "policy_head": scatter_about(splits[1], (D, V), D ** -0.5, 0.0625, ((1, 32),)),
        "reference_head": scatter_about(splits[2], (D, V), D ** -0.5, 0.0625, ((1, 32),)),
        "targets": plant(ranked_ids(splits[3], (TOKENS,), V, 2), jax.random.fold_in(splits[3], 3), 0, V - 1).astype(jnp.int32),
    }


def reference(hidden, policy_head, reference_head, targets):
    policy_logits = jnp.dot(hidden, policy_head, preferred_element_type=jnp.float32)
    reference_logits = jnp.dot(hidden, reference_head, preferred_element_type=jnp.float32)
    peak_policy = jnp.max(policy_logits, axis=1)
    peak_reference = jnp.max(reference_logits, axis=1)
    policy_exp = jnp.exp(policy_logits - peak_policy[:, None])
    total_policy = jnp.sum(policy_exp, axis=1)
    total_reference = jnp.sum(jnp.exp(reference_logits - peak_reference[:, None]), axis=1)
    weighted = jnp.sum(policy_exp * (policy_logits - reference_logits), axis=1)
    vocab_ids = jnp.arange(policy_logits.shape[1], dtype=jnp.int32)
    target_hits = vocab_ids[None, :] == targets.astype(jnp.int32)[:, None]
    target_policy = jnp.sum(jnp.where(target_hits, policy_logits, jnp.zeros_like(policy_logits)), axis=1)
    target_reference = jnp.sum(jnp.where(target_hits, reference_logits, jnp.zeros_like(reference_logits)), axis=1)
    log_norm_policy = peak_policy + jnp.log(total_policy)
    log_norm_reference = peak_reference + jnp.log(total_reference)
    policy_logprob = target_policy - log_norm_policy
    reference_logprob = target_reference - log_norm_reference
    divergence = weighted / total_policy - log_norm_policy + log_norm_reference
    return (policy_logprob, reference_logprob, divergence)
```

```python
import functools

import jax
import jax.numpy as jnp
from jax import lax
from jax.experimental import pallas as pl
from jax.experimental.pallas import tpu as pltpu
from jax.sharding import PartitionSpec as P

MESH = pl.DeviceIdType.MESH
TILE = 256


def kernel(T, V, hid, wp, wr, tgt, o0, o1, o2, h, w, acc, tg, st, got,
           wsem, osem, rs, rr, xs, xr, cs, cr, ts, tr, es, er):
    R = hid.shape[0]
    D = hid.shape[1]
    C = wp.shape[1]
    M = T * R
    Kp = D // 6
    t = lax.axis_index("tok")
    v = lax.axis_index("vocab")
    core = lax.rem(v, 2)
    xb = lax.rem(v // 2, 2)
    partner = v + 1 - 2 * core
    twin = v + 2 - 4 * xb
    half = T // 2
    pos = jnp.where(lax.rem(t, 2) == 0, t // 2, T - 1 - t // 2)

    def tok_at(p):
        p = lax.rem(p + 2 * T, T)
        return jnp.where(p < half, 2 * p, 2 * (T - 1 - p) + 1)

    right, left = tok_at(pos + 1), tok_at(pos - 1)

    def part(c, kind):
        if kind == 0:
            return 3 * c
        return 3 * c + 1 + (xb if kind == 1 else 1 - xb)

    order = [(0, 0), (1, 0), (0, 1), (1, 1), (0, 2), (1, 2)]

    def cols(p):
        return pl.ds(pl.multiple_of(p * Kp, 128), Kp)

    own = pltpu.make_async_copy(hid, h.at[t], osem)
    own.start()
    wcopies = []
    for i, (c, kind) in enumerate(order):
        k = cols(part(c, kind))
        wcopies.append([
            pltpu.make_async_copy(wp.at[k, :], w.at[k, pl.ds(0, C)], wsem.at[0, i]),
            pltpu.make_async_copy(wr.at[k, :], w.at[k, pl.ds(C, C)], wsem.at[1, i]),
        ])

    barrier = pltpu.get_barrier_semaphore()

    def greet(j, _):
        q = lax.rem(t * V + v + j, T * V)
        pl.semaphore_signal(barrier, inc=1, device_id=(q // V, lax.rem(q, V)), device_id_type=MESH)
        return 0

    lax.fori_loop(1, T * V, greet, 0)
    for pair in wcopies:
        for cp in pair:
            cp.start()

    rowi = lax.broadcasted_iota(jnp.int32, (R, 128), 0)
    tv = jnp.zeros((R, 128), jnp.int32)
    for i in range(R):
        tv = jnp.where(rowi == i, tgt[i], tv)
    tg[t] = tv
    own.wait()
    pl.semaphore_wait(barrier, T * V - 1)

    counts = {(0, 0): half, (0, 1): T - 1 - half, (1, 0): T - 1 - half, (1, 1): half}
    sends = []

    def ring(kind, d, n):
        src = tok_at(pos - n) if d == 0 else tok_at(pos + n)
        blk = h.at[src, :, cols(part(core, kind))]
        return pltpu.make_async_remote_copy(
            src_ref=blk, dst_ref=blk, send_sem=rs.at[kind, d, n], recv_sem=rr.at[kind, d, n],
            device_id=(right if d == 0 else left, v), device_id_type=MESH)

    def landed(d, n):
        return tok_at(pos - 1 - n) if d == 0 else tok_at(pos + 1 + n)

    def cross(kind, d, n):
        blk = h.at[landed(d, n), :, cols(part(core, kind))]
        return pltpu.make_async_remote_copy(
            src_ref=blk, dst_ref=blk, send_sem=xs.at[d, n], recv_sem=xr.at[d, n],
            device_id=(t, twin), device_id_type=MESH)

    def pairwise(c, kind, dd, n):
        blk = h.at[landed(dd, n), :, cols(part(c, kind))]
        return pltpu.make_async_remote_copy(
            src_ref=blk, dst_ref=blk, send_sem=cs.at[kind, dd, n], recv_sem=cr.at[kind, dd, n],
            device_id=(t, partner), device_id_type=MESH)

    def go(cp):
        cp.start()
        sends.append(cp)

    xcounts = {0: counts[(1, 0)], 1: counts[(1, 1)]}

    for n in range(half + 1):
        for kind in (1, 0):
            for d in (0, 1):
                cnt = counts[(kind, d)]
                if 1 <= n <= cnt:
                    ring(kind, d, n - 1).wait_recv()
                if n < cnt:
                    go(ring(kind, d, n))
                if 1 <= n <= cnt:
                    if kind == 1:
                        go(cross(1, d, n - 1))
                    go(pairwise(core, kind, d, n - 1))
        if n == 0:
            for j in range(1, T):
                go(pltpu.make_async_remote_copy(
                    src_ref=tg.at[t], dst_ref=tg.at[t], send_sem=ts.at[j], recv_sem=tr.at[j],
                    device_id=(lax.rem(t + j, T), v), device_id_type=MESH))
        if n >= 3:
            for d in (0, 1):
                if n - 3 < xcounts[d]:
                    cross(2, d, n - 3).wait_recv()
                    go(pairwise(core, 2, d, n - 3))

    def matmul(i):
        c, kind = order[i]
        k = cols(part(c, kind))
        for cp in wcopies[i]:
            cp.wait()
        a = h[:, :, k].reshape(M, Kp)

        def tile(j, _):
            nn = pl.ds(pl.multiple_of(j * TILE, TILE), TILE)
            y = jnp.dot(a, w[k, nn], preferred_element_type=jnp.float32)
            if i == 0:
                acc[:, nn] = y
            else:
                acc[:, nn] += y
            return 0

        lax.fori_loop(0, 2 * C // TILE, tile, 0)

    def wait_pair(kind):
        for d in (0, 1):
            cnt = counts[(min(kind, 1), d)]
            for n in range(cnt):
                pairwise(1 - core, kind, d, n).wait_recv()

    wait_pair(0)
    matmul(0)
    matmul(1)
    for n in range(half):
        for d in (0, 1):
            if max(half - 2, 0) <= n < xcounts[d]:
                cross(2, d, n).wait_recv()
                go(pairwise(core, 2, d, n))
    wait_pair(1)
    matmul(2)
    matmul(3)
    wait_pair(2)
    matmul(4)
    matmul(5)

    for j in range(1, T):
        src = lax.rem(t - j + T, T)
        pltpu.make_async_remote_copy(
            src_ref=tg.at[src], dst_ref=tg.at[src], send_sem=ts.at[j], recv_sem=tr.at[j],
            device_id=(src, v), device_id_type=MESH).wait_recv()

    me = t * V + v
    base = me * C
    for q in range(T):
        rows = pl.ds(q * R, R)
        lp = acc[rows, pl.ds(0, C)]
        lr = acc[rows, pl.ds(C, C)]
        ids = lax.broadcasted_iota(jnp.int32, (R, C), 1) + base
        hit = ids == tg[q][:, 0:1]
        pp = jnp.max(lp, axis=1, keepdims=True)
        pr = jnp.max(lr, axis=1, keepdims=True)
        ep = jnp.exp(lp - pp)
        er_ = jnp.exp(lr - pr)
        parts = [
            pp, pr,
            jnp.sum(ep, axis=1, keepdims=True),
            jnp.sum(er_, axis=1, keepdims=True),
            jnp.sum(ep * (lp - lr), axis=1, keepdims=True),
            jnp.sum(jnp.where(hit, lp, 0.0), axis=1, keepdims=True),
            jnp.sum(jnp.where(hit, lr, 0.0), axis=1, keepdims=True),
        ]
        lane = lax.broadcasted_iota(jnp.int32, (R, 128), 1)
        s = jnp.zeros((R, 128), jnp.float32)
        for i, value in enumerate(parts):
            s = jnp.where(lane == i, value, s)
        s = jnp.concatenate([s, jnp.zeros((128 - R, 128), jnp.float32)], axis=0)
        st[q] = s.T[0:8, :]

    got[me] = st[t]

    def spread(j, _):
        q = lax.rem(me + j, T * V)
        qt, qv = q // V, lax.rem(q, V)
        pltpu.make_async_remote_copy(
            src_ref=st.at[qt], dst_ref=got.at[me], send_sem=es.at[j], recv_sem=er.at[j],
            device_id=(qt, qv), device_id_type=MESH).start()
        return 0

    lax.fori_loop(1, T * V, spread, 0)
    for cp in sends:
        cp.wait_send()

    def collect(j, _):
        q = lax.rem(me - j + T * V, T * V)
        cp = pltpu.make_async_remote_copy(
            src_ref=st.at[t], dst_ref=got.at[q], send_sem=es.at[j], recv_sem=er.at[j],
            device_id=(q // V, lax.rem(q, V)), device_id_type=MESH)
        cp.wait_recv()
        cp.wait_send()
        return 0

    lax.fori_loop(1, T * V, collect, 0)

    g = got[...]
    top = jnp.max(g, axis=0)
    scale = jnp.exp(g - top[None])
    pp, pr = top[0:1], top[1:2]
    sp, sr = scale[:, 0:1, :], scale[:, 1:2, :]
    tp = jnp.sum(g[:, 2:3, :] * sp, axis=0)
    tt = jnp.sum(g[:, 3:4, :] * sr, axis=0)
    wt = jnp.sum(g[:, 4:5, :] * sp, axis=0)
    hp = jnp.sum(g[:, 5:6, :], axis=0)
    hr = jnp.sum(g[:, 6:7, :], axis=0)
    np_ = pp + jnp.log(tp)
    nr = pr + jnp.log(tt)
    o0[...] = (hp - np_)[0, :R]
    o1[...] = (hr - nr)[0, :R]
    o2[...] = (wt / tp - np_ + nr)[0, :R]


def solution(mesh):
    T, V = mesh.shape["tok"], mesh.shape["vocab"]

    def body(hidden, policy_head, reference_head, targets):
        R, D = hidden.shape
        C = policy_head.shape[1]
        half = T // 2
        dma = pltpu.SemaphoreType.DMA
        anyspec = pl.BlockSpec(memory_space=pl.ANY)
        vm = pl.BlockSpec(memory_space=pltpu.VMEM)
        out = jax.ShapeDtypeStruct((R,), jnp.float32)
        return pl.pallas_call(
            functools.partial(kernel, T, V),
            out_shape=(out, out, out),
            in_specs=[anyspec, anyspec, anyspec, pl.BlockSpec(memory_space=pltpu.SMEM)],
            out_specs=(vm, vm, vm),
            scratch_shapes=[
                pltpu.VMEM((T, R, D), jnp.bfloat16),
                pltpu.VMEM((D, 2 * C), jnp.bfloat16),
                pltpu.VMEM((T * R, 2 * C), jnp.float32),
                pltpu.VMEM((T, R, 128), jnp.int32),
                pltpu.VMEM((T, 8, 128), jnp.float32),
                pltpu.VMEM((T * V, 8, 128), jnp.float32),
                dma((2, 6)),
                dma,
                dma((2, 2, half)),
                dma((2, 2, half)),
                dma((2, half)),
                dma((2, half)),
                dma((3, 2, half)),
                dma((3, 2, half)),
                dma((T,)),
                dma((T,)),
                dma((T * V,)),
                dma((T * V,)),
            ],
            compiler_params=pltpu.CompilerParams(
                collective_id=0, has_side_effects=True, vmem_limit_bytes=67043328),
        )(hidden, policy_head, reference_head, targets)

    in_specs = (P("tok", None), P(None, ("tok", "vocab")), P(None, ("tok", "vocab")), P("tok"))
    out_specs = (P("tok"), P("tok"), P("tok"))
    return jax.shard_map(body, mesh=mesh, in_specs=in_specs, out_specs=out_specs, check_vma=False)
```

```python
import functools

import jax
import jax.numpy as jnp
from jax import lax
from jax.experimental import pallas as pl
from jax.experimental.pallas import tpu as pltpu
from jax.sharding import PartitionSpec as P

MESH = pl.DeviceIdType.MESH
TILE = 2048


def kernel(T, V, hid, wp, wr, tgt, o, h, w, flat, acc, tg, st, got,
           wsem, osem, rs, rr, xs, xr, cs, cr, ts, tr, es, er):
    R = hid.shape[0]
    D = hid.shape[1]
    C = wp.shape[1]
    M = T * R
    Kp = D // 6
    t = lax.axis_index("tok")
    v = lax.axis_index("vocab")
    core = lax.rem(v, 2)
    xb = lax.rem(v // 2, 2)
    partner = v + 1 - 2 * core
    twin = v + 2 - 4 * xb
    half = T // 2
    pos = jnp.where(lax.rem(t, 2) == 0, t // 2, T - 1 - t // 2)

    def tok_at(p):
        p = lax.rem(p + 2 * T, T)
        return jnp.where(p < half, 2 * p, 2 * (T - 1 - p) + 1)

    right, left = tok_at(pos + 1), tok_at(pos - 1)

    def part(c, kind):
        if kind == 0:
            return 3 * c
        return 3 * c + 1 + (xb if kind == 1 else 1 - xb)

    order = [(core, 0), (core, 1), (1 - core, 0), (1 - core, 1), (core, 2), (1 - core, 2)]

    def cols(p):
        return pl.ds(pl.multiple_of(p * Kp, 128), Kp)

    own = pltpu.make_async_copy(hid, h.at[t], osem)
    own.start()
    wcopies = []
    for i, (c, kind) in enumerate(order):
        k = cols(part(c, kind))
        wcopies.append([
            pltpu.make_async_copy(wp.at[k, :], w.at[k, pl.ds(0, C)], wsem.at[0, i]),
            pltpu.make_async_copy(wr.at[k, :], w.at[k, pl.ds(C, C)], wsem.at[1, i]),
        ])

    barrier = pltpu.get_barrier_semaphore()

    def greet(j, _):
        q = lax.rem(t * V + v + j, T * V)
        pl.semaphore_signal(barrier, inc=1, device_id=(q // V, lax.rem(q, V)), device_id_type=MESH)
        return 0

    lax.fori_loop(1, T * V, greet, 0)
    for pair in wcopies:
        for cp in pair:
            cp.start()

    rowi = lax.broadcasted_iota(jnp.int32, (R, 128), 0)
    tv = jnp.zeros((R, 128), jnp.int32)
    for i in range(R):
        tv = jnp.where(rowi == i, tgt[i], tv)
    tg[t] = tv
    own.wait()
    pl.semaphore_wait(barrier, T * V - 1)

    counts = {(0, 0): half, (0, 1): T - 1 - half, (1, 0): T - 1 - half, (1, 1): half}
    sends = []

    def ring(kind, d, n):
        src = tok_at(pos - n) if d == 0 else tok_at(pos + n)
        blk = h.at[src, :, cols(part(core, kind))]
        return pltpu.make_async_remote_copy(
            src_ref=blk, dst_ref=blk, send_sem=rs.at[kind, d, n], recv_sem=rr.at[kind, d, n],
            device_id=(right if d == 0 else left, v), device_id_type=MESH)

    def landed(d, n):
        return tok_at(pos - 1 - n) if d == 0 else tok_at(pos + 1 + n)

    def cross(kind, d, n):
        blk = h.at[landed(d, n), :, cols(part(core, kind))]
        return pltpu.make_async_remote_copy(
            src_ref=blk, dst_ref=blk, send_sem=xs.at[d, n], recv_sem=xr.at[d, n],
            device_id=(t, twin), device_id_type=MESH)

    def pairwise(c, kind, dd, n):
        blk = h.at[landed(dd, n), :, cols(part(c, kind))]
        return pltpu.make_async_remote_copy(
            src_ref=blk, dst_ref=blk, send_sem=cs.at[kind, dd, n], recv_sem=cr.at[kind, dd, n],
            device_id=(t, partner), device_id_type=MESH)

    def go(cp):
        cp.start()
        sends.append(cp)

    xcounts = {0: counts[(1, 0)], 1: counts[(1, 1)]}

    for n in range(half + 1):
        for kind in (1, 0):
            for d in (0, 1):
                cnt = counts[(kind, d)]
                if 1 <= n <= cnt:
                    ring(kind, d, n - 1).wait_recv()
                if n < cnt:
                    go(ring(kind, d, n))
                if 1 <= n <= cnt:
                    if kind == 1:
                        go(cross(1, d, n - 1))
                    go(pairwise(core, kind, d, n - 1))
        if n == 0:
            for j in range(1, T):
                go(pltpu.make_async_remote_copy(
                    src_ref=tg.at[t], dst_ref=tg.at[t], send_sem=ts.at[j], recv_sem=tr.at[j],
                    device_id=(lax.rem(t + j, T), v), device_id_type=MESH))
        if n >= 3:
            for d in (0, 1):
                if n - 3 < xcounts[d]:
                    cross(2, d, n - 3).wait_recv()
                    go(pairwise(core, 2, d, n - 3))

    def matmul(i):
        c, kind = order[i]
        k = cols(part(c, kind))
        for cp in wcopies[i]:
            cp.wait()
        for q in range(T):
            flat[pl.ds(q * R, R), :] = h[q, :, k]

        wide = min(TILE, 2 * C)

        def tile(j, _):
            nn = pl.ds(pl.multiple_of(j * wide, wide), wide)
            y = jnp.dot(flat[...], w[k, nn], preferred_element_type=jnp.float32)
            if i == 0:
                acc[:, nn] = y
            else:
                acc[:, nn] += y
            return 0

        lax.fori_loop(0, 2 * C // wide, tile, 0)

    def wait_pair(kind):
        for d in (0, 1):
            cnt = counts[(min(kind, 1), d)]
            for n in range(cnt):
                pairwise(1 - core, kind, d, n).wait_recv()

    matmul(0)
    for n in range(half):
        for d in (0, 1):
            if max(half - 2, 0) <= n < xcounts[d]:
                cross(2, d, n).wait_recv()
                go(pairwise(core, 2, d, n))
    matmul(1)
    wait_pair(0)
    matmul(2)
    wait_pair(1)
    matmul(3)
    matmul(4)
    wait_pair(2)
    matmul(5)

    for j in range(1, T):
        src = lax.rem(t - j + T, T)
        pltpu.make_async_remote_copy(
            src_ref=tg.at[src], dst_ref=tg.at[src], send_sem=ts.at[j], recv_sem=tr.at[j],
            device_id=(src, v), device_id_type=MESH).wait_recv()

    me = t * V + v
    base = me * C
    for q in range(T):
        rows = pl.ds(q * R, R)
        lp = acc[rows, pl.ds(0, C)]
        lr = acc[rows, pl.ds(C, C)]
        ids = lax.broadcasted_iota(jnp.int32, (R, C), 1) + base
        hit = ids == tg[q][:, 0:1]
        pp = jnp.max(lp, axis=1, keepdims=True)
        pr = jnp.max(lr, axis=1, keepdims=True)
        ep = jnp.exp(lp - pp)
        er_ = jnp.exp(lr - pr)
        parts = [
            pp, pr,
            jnp.sum(ep, axis=1, keepdims=True),
            jnp.sum(er_, axis=1, keepdims=True),
            jnp.sum(ep * (lp - lr), axis=1, keepdims=True),
            jnp.sum(jnp.where(hit, lp, 0.0), axis=1, keepdims=True),
            jnp.sum(jnp.where(hit, lr, 0.0), axis=1, keepdims=True),
        ]
        lane = lax.broadcasted_iota(jnp.int32, (R, 128), 1)
        s = jnp.zeros((R, 128), jnp.float32)
        for i, value in enumerate(parts):
            s = jnp.where(lane == i, value, s)
        s = jnp.concatenate([s, jnp.zeros((128 - R, 128), jnp.float32)], axis=0)
        st[q] = s.T[0:8, :]

    got[me] = st[t]

    def spread(j, _):
        q = lax.rem(me + j, T * V)
        qt, qv = q // V, lax.rem(q, V)
        pltpu.make_async_remote_copy(
            src_ref=st.at[qt], dst_ref=got.at[me], send_sem=es.at[j], recv_sem=er.at[j],
            device_id=(qt, qv), device_id_type=MESH).start()
        return 0

    lax.fori_loop(1, T * V, spread, 0)
    for cp in sends:
        cp.wait_send()

    def collect(j, _):
        q = lax.rem(me - j + T * V, T * V)
        cp = pltpu.make_async_remote_copy(
            src_ref=st.at[t], dst_ref=got.at[q], send_sem=es.at[j], recv_sem=er.at[j],
            device_id=(q // V, lax.rem(q, V)), device_id_type=MESH)
        cp.wait_recv()
        cp.wait_send()
        return 0

    lax.fori_loop(1, T * V, collect, 0)

    g = got[...]
    top = jnp.max(g, axis=0)
    scale = jnp.exp(g - top[None])
    pp, pr = top[0:1], top[1:2]
    sp, sr = scale[:, 0:1, :], scale[:, 1:2, :]
    tp = jnp.sum(g[:, 2:3, :] * sp, axis=0)
    tt = jnp.sum(g[:, 3:4, :] * sr, axis=0)
    wt = jnp.sum(g[:, 4:5, :] * sp, axis=0)
    hp = jnp.sum(g[:, 5:6, :], axis=0)
    hr = jnp.sum(g[:, 6:7, :], axis=0)
    np_ = pp + jnp.log(tp)
    nr = pr + jnp.log(tt)
    o[...] = jnp.concatenate([hp - np_, hr - nr, wt / tp - np_ + nr], axis=0)


def solution(mesh):
    T, V = mesh.shape["tok"], mesh.shape["vocab"]

    def body(hidden, policy_head, reference_head, targets):
        R, D = hidden.shape
        C = policy_head.shape[1]
        half = T // 2
        dma = pltpu.SemaphoreType.DMA
        anyspec = pl.BlockSpec(memory_space=pl.ANY)
        vm = pl.BlockSpec(memory_space=pltpu.VMEM)
        out = jax.ShapeDtypeStruct((3, 128), jnp.float32)
        o = pl.pallas_call(
            functools.partial(kernel, T, V),
            out_shape=out,
            in_specs=[anyspec, anyspec, anyspec, pl.BlockSpec(memory_space=pltpu.SMEM)],
            out_specs=vm,
            scratch_shapes=[
                pltpu.VMEM((T, R, D), jnp.bfloat16),
                pltpu.VMEM((D, 2 * C), jnp.bfloat16),
                pltpu.VMEM((T * R, D // 6), jnp.bfloat16),
                pltpu.VMEM((T * R, 2 * C), jnp.float32),
                pltpu.VMEM((T, R, 128), jnp.int32),
                pltpu.VMEM((T, 8, 128), jnp.float32),
                pltpu.VMEM((T * V, 8, 128), jnp.float32),
                dma((2, 6)),
                dma,
                dma((2, 2, half)),
                dma((2, 2, half)),
                dma((2, half)),
                dma((2, half)),
                dma((3, 2, half)),
                dma((3, 2, half)),
                dma((T,)),
                dma((T,)),
                dma((T * V,)),
                dma((T * V,)),
            ],
            compiler_params=pltpu.CompilerParams(
                collective_id=0, has_side_effects=True, vmem_limit_bytes=67043328),
        )(hidden, policy_head, reference_head, targets)
        return o[0, :R], o[1, :R], o[2, :R]

    in_specs = (P("tok", None), P(None, ("tok", "vocab")), P(None, ("tok", "vocab")), P("tok"))
    out_specs = (P("tok"), P("tok"), P("tok"))
    return jax.shard_map(body, mesh=mesh, in_specs=in_specs, out_specs=out_specs, check_vma=False)
```
